32 devices in a mesh: freq: 2 (over x), panel: 16 (over z, y, core).
Axes of the slice: x: 2, y: 2, z: 4, core: 2. Of those that a mesh axis runs over, the one named last changes fastest.
Arguments:
- recorded: float32 [2, 2, 2048, 2048], P('freq', None, 'panel'), parts along dimension 0, may hold values from -60 to 60
- receiver_kernel: bfloat16 [2, 2, 4095], P('freq'), parts along dimension 0, may hold values from -1.5 to 1.5
- source_kernel: bfloat16 [2, 2, 4095], P('freq'), parts along dimension 0, may hold values from -1.5 to 1.5
Outputs:
- primaries: float32 [2, 2, 2048, 2048], P('freq', None, 'panel'), parts along dimension 0
- multiples: bfloat16 [2, 2, 2048, 2048], P('freq', None, 'panel'), parts along dimension 0
The draws below stay inside these ranges and needn't reach their ends.
There are 2 independent parts, one for each index of `freq`. The reference program is written for one: setup_inputs(seed, part) draws one part's arguments, and reference() takes and returns one part's arrays. A program takes and returns all parts, laid end to end along the dimension named above; each array names one. Nothing has to cross between parts.
All inputs are finite; a program needn't handle non-finite values.
Results may differ from the reference program's by a relative error of at most 0.0057.
Values may be sent and summed in bfloat16 or wider, within the bound.
A program may use at most 320 MiB of HBM per device.

```python
import math
import jax
import jax.numpy as jnp

FREQS = 1
NS = 2048
NR = 2048


def focal_kernel(key, width):
    key_taps, key_phase, key_mag = jax.random.split(key, 3)
    count = 2 * width - 1
    taps = jnp.clip(jax.random.normal(key_taps, (FREQS, 2, count), jnp.float32), -6.0, 6.0)
    taps = taps / jnp.sqrt(2.0 * width)
    phase = jax.random.uniform(key_phase, (FREQS, 1), jnp.float32, -math.pi, math.pi)
    magnitude = jax.random.uniform(key_mag, (FREQS, 1), jnp.float32, 0.8, 1.2)
    center = (jnp.arange(count) == width - 1)[None, :]
    real_part = jnp.where(center, magnitude * jnp.cos(phase), taps[:, 0])
    imag_part = jnp.where(center, magnitude * jnp.sin(phase), taps[:, 1])
    return jnp.stack([real_part, imag_part], axis=1).astype(jnp.bfloat16)


def draw_receiver_kernel(key, part):
    return focal_kernel(jax.random.fold_in(key, 11), NR)


def draw_source_kernel(key, part):
    return focal_kernel(jax.random.fold_in(key, 23), NS)


def draw_recorded(key, part):
    key_base, key_rows, key_cols = jax.random.split(jax.random.fold_in(key, 37), 3)
    rising = 3.0 ** (jnp.arange(NS, dtype=jnp.float32) / (NS - 1))
    base = jnp.clip(jax.random.normal(key_base, (FREQS, 2, NS, NR), jnp.float32), -6.0, 6.0)
    row_scale = jnp.exp(jax.random.uniform(key_rows, (NS,), jnp.float32, math.log(0.7), math.log(1.4)))
    col_scale = jnp.exp(jax.random.uniform(key_cols, (NR,), jnp.float32, math.log(0.7), math.log(1.4)))
    return base * (rising * row_scale)[:, None] * col_scale[None, :]


def setup_inputs(seed: int = 0, part: int = 0) -> dict:
    keys = jax.random.split(jax.random.key(seed), 4)
    part_splits = jax.random.split(jax.random.fold_in(keys[3], part), 4)
    return {
        "recorded": draw_recorded(jax.random.fold_in(jax.random.fold_in(keys[3], part), 71), part),
        "receiver_kernel": draw_receiver_kernel(jax.random.fold_in(jax.random.fold_in(keys[3], part), 71), part),
        "source_kernel": draw_source_kernel(jax.random.fold_in(jax.random.fold_in(keys[3], part), 71), part),
    }


def toeplitz(kernel, width):
    rows = jnp.arange(width, dtype=jnp.int32)[:, None]
    cols = jnp.arange(width, dtype=jnp.int32)[None, :]
    return kernel[:, cols - rows + width - 1]


def complex_dot(left, right):
    real_part = jnp.dot(left[0], right[0], preferred_element_type=jnp.float32) - jnp.dot(left[1], right[1], preferred_element_type=jnp.float32)
    imag_part = jnp.dot(left[0], right[1], preferred_element_type=jnp.float32) + jnp.dot(left[1], right[0], preferred_element_type=jnp.float32)
    return jnp.stack([real_part, imag_part])


def reference(recorded, receiver_kernel, source_kernel):
    prim_list = []
    mult_list = []
    for slot in range(FREQS):
        data = recorded[slot]
        data_b = data.astype(jnp.bfloat16)
        g_recv = toeplitz(receiver_kernel[slot], NR)
        g_src = toeplitz(source_kernel[slot], NS)
        focused = complex_dot(data_b, g_recv).astype(jnp.bfloat16)
        mult = complex_dot(g_src, focused).astype(jnp.bfloat16)
        mfl = mult.astype(jnp.float32)
        num_re = jnp.sum(mfl[0] * data[0] + mfl[1] * data[1])
        num_im = jnp.sum(mfl[0] * data[1] - mfl[1] * data[0])
        den = jnp.sum(mfl[0] * mfl[0] + mfl[1] * mfl[1]) + 1e-6
        fit_re = num_re / den
        fit_im = num_im / den
        prim_re = data[0] - (fit_re * mfl[0] - fit_im * mfl[1])
        prim_im = data[1] - (fit_re * mfl[1] + fit_im * mfl[0])
        prim_list.append(jnp.stack([prim_re, prim_im]))
        mult_list.append(mult)
    return jnp.stack(prim_list), jnp.stack(mult_list)
```

```python
import functools

import jax
import jax.numpy as jnp
from jax import lax
from jax.experimental import pallas as pl
from jax.experimental.pallas import tpu as pltpu
from jax.sharding import PartitionSpec as P

MESH = pl.DeviceIdType.MESH
LANES = 128
GROUP = 256
STRIP = 16


def skew(taps_ref, comp, block, lane0, band_ref):
    length = taps_ref.shape[1]
    x = jnp.broadcast_to(taps_ref[comp : comp + 1, :], (STRIP, length))
    row = lax.broadcasted_iota(jnp.int32, (STRIP, length), 0)
    step = 1
    while step < STRIP:
        x = jnp.where((row & step) != 0, pltpu.roll(x, step, 1), x)
        step *= 2
    for s in range(0, LANES, STRIP):
        shift = (s - (LANES - block)) % length
        y = (pltpu.roll(x, shift, 1) if shift else x).astype(jnp.bfloat16)
        for m in range(length // LANES):
            at = length - LANES * (m + 1)
            band_ref[m * LANES + s : m * LANES + s + STRIP, lane0 : lane0 + block] = y[:, at : at + block]


def exchange_kernel(
    panels,
    rec_ref,
    rtaps_ref,
    staps_ref,
    mult_ref,
    fit_ref,
    band_r,
    band_s,
    w1,
    w2,
    foc,
    foc_in,
    mul,
    mul_in,
    sums,
    sums_in,
    send1,
    recv1,
    send2,
    recv2,
    send3,
    recv3,
):
    me = lax.axis_index("panel")
    rows, width = rec_ref.shape[2], rec_ref.shape[3]
    sources = rows * panels
    cols = width // panels
    nt = (((1,), (1,)), ((), ()))

    def peer(o):
        return lax.rem(me + o, panels)

    barrier = pltpu.get_barrier_semaphore()

    @pl.loop(1, panels)
    def _(o):
        pl.semaphore_signal(barrier, inc=1, device_id={"panel": peer(o)}, device_id_type=MESH)

    for kb in range(width // LANES):
        re = rec_ref[0, 0, :, kb * LANES : (kb + 1) * LANES].astype(jnp.bfloat16)
        im = rec_ref[0, 1, :, kb * LANES : (kb + 1) * LANES].astype(jnp.bfloat16)
        at = 2 * kb * LANES
        w1[0:rows, at : at + LANES] = re
        w1[0:rows, at + LANES : at + 2 * LANES] = -im
        w1[rows : 2 * rows, at : at + LANES] = im
        w1[rows : 2 * rows, at + LANES : at + 2 * LANES] = re
    skew(rtaps_ref, 0, LANES, 0, band_r)
    skew(rtaps_ref, 1, LANES, LANES, band_r)

    pl.semaphore_wait(barrier, panels - 1)

    def copy1(dest, src):
        return pltpu.make_async_remote_copy(
            src_ref=foc.at[pl.ds(pl.multiple_of(dest * cols, cols), cols), :],
            dst_ref=foc_in.at[src],
            send_sem=send1.at[dest],
            recv_sem=recv1.at[src],
            device_id={"panel": dest},
            device_id_type=MESH,
        )

    def copy2(dest, src):
        return pltpu.make_async_remote_copy(
            src_ref=mul.at[pl.ds(pl.multiple_of(dest * rows, rows), rows), :],
            dst_ref=mul_in.at[src],
            send_sem=send2.at[dest],
            recv_sem=recv2.at[src],
            device_id={"panel": dest},
            device_id_type=MESH,
        )

    def copy3(dest, src):
        return pltpu.make_async_remote_copy(
            src_ref=sums,
            dst_ref=sums_in.at[src],
            send_sem=send3.at[dest],
            recv_sem=recv3.at[src],
            device_id={"panel": dest},
            device_id_type=MESH,
        )

    groups1 = width // GROUP
    per1 = GROUP // cols
    own1 = me // per1

    @pl.loop(0, groups1)
    def _(n):
        g = lax.rem(own1 + 1 + n, groups1)
        first = pl.multiple_of(g * GROUP, GROUP)
        lhs = jnp.concatenate(
            [
                band_r[pl.ds(pl.multiple_of(width - LANES * (kb + 1) + first, LANES), GROUP), :]
                for kb in range(width // LANES)
            ],
            axis=1,
        )
        out = lax.dot_general(lhs, w1[...], nt, preferred_element_type=jnp.float32)
        foc[pl.ds(first, GROUP), :] = out.astype(jnp.bfloat16)
        for d in range(per1):
            dest = g * per1 + d

            @pl.when(dest != me)
            def _():
                copy1(dest, me).start()

    foc_in[me] = foc[pl.ds(pl.multiple_of(me * cols, cols), cols), :]
    skew(staps_ref, 0, rows, 0, band_s)
    skew(staps_ref, 1, rows, rows, band_s)

    @pl.loop(1, panels)
    def _(o):
        copy1(peer(o), peer(o)).wait_recv()

    lane = lax.broadcasted_iota(jnp.int32, (cols, 2 * rows), 1)
    for j in range(panels):
        x = foc_in[j]
        at = 2 * rows * j
        w2[0:cols, at : at + 2 * rows] = jnp.where(lane < rows, x, -x)
        w2[cols : 2 * cols, at : at + 2 * rows] = jnp.concatenate([x[:, rows:], x[:, :rows]], axis=1)

    groups2 = sources // GROUP
    per2 = GROUP // rows
    own2 = me // per2

    @pl.loop(0, groups2)
    def _(n):
        g = lax.rem(own2 + 1 + n, groups2)
        first = pl.multiple_of(g * GROUP, GROUP)
        lhs = jnp.concatenate(
            [
                band_s[pl.ds(pl.multiple_of(sources - rows * (jb + 1) + first, rows), GROUP), :]
                for jb in range(panels)
            ],
            axis=1,
        )
        out = lax.dot_general(lhs, w2[...], nt, preferred_element_type=jnp.float32)
        mul[pl.ds(first, GROUP), :] = out.astype(jnp.bfloat16)
        for d in range(per2):
            dest = g * per2 + d

            @pl.when(dest != me)
            def _():
                copy2(dest, me).start()

    mul_in[me] = mul[pl.ds(pl.multiple_of(me * rows, rows), rows), :]

    @pl.loop(1, panels)
    def _(o):
        copy2(peer(o), peer(o)).wait_recv()

    def fold(v):
        return jnp.sum(v, axis=0, keepdims=True)

    num_re = jnp.zeros((1, LANES), jnp.float32)
    num_im = jnp.zeros((1, LANES), jnp.float32)
    energy = jnp.zeros((1, LANES), jnp.float32)
    per = LANES // cols
    for cb in range(width // LANES):
        blocks = [mul_in[cb * per + d] for d in range(per)]
        mre = jnp.concatenate([b[:, :cols] for b in blocks], axis=1)
        mim = jnp.concatenate([b[:, cols:] for b in blocks], axis=1)
        at = cb * LANES
        mult_ref[0, 0, :, at : at + LANES] = mre
        mult_ref[0, 1, :, at : at + LANES] = mim
        mre = mre.astype(jnp.float32)
        mim = mim.astype(jnp.float32)
        pre = rec_ref[0, 0, :, at : at + LANES]
        pim = rec_ref[0, 1, :, at : at + LANES]
        num_re += fold(mre * pre + mim * pim)
        num_im += fold(mre * pim - mim * pre)
        energy += fold(mre * mre + mim * mim)
    part = jnp.concatenate([num_re, num_im, energy, jnp.zeros((5, LANES), jnp.float32)], axis=0)
    sums[...] = part
    sums_in[me] = part

    @pl.loop(1, panels)
    def _(o):
        copy3(peer(o), me).start()

    @pl.loop(1, panels)
    def _(o):
        copy1(peer(o), me).wait_send()
        copy2(peer(o), me).wait_send()

    @pl.loop(1, panels)
    def _(o):
        copy3(peer(o), peer(o)).wait_recv()

    @pl.loop(1, panels)
    def _(o):
        copy3(peer(o), me).wait_send()

    total = jnp.sum(jnp.sum(sums_in[...], axis=0), axis=1, keepdims=True)
    fit = total[0:2, :] / (total[2:3, :] + 1e-06)
    fit_ref[...] = jnp.broadcast_to(
        jnp.concatenate([fit, jnp.zeros((6, 1), jnp.float32)], axis=0), (8, LANES)
    )


def subtract_kernel(rec_ref, mult_in_ref, fit_ref, prim_ref, mult_ref):
    fit_re = fit_ref[0:1, 0:1]
    fit_im = fit_ref[1:2, 0:1]
    mult_ref[...] = mult_in_ref[...]
    mre = mult_in_ref[0, 0].astype(jnp.float32)
    mim = mult_in_ref[0, 1].astype(jnp.float32)
    prim_ref[0, 0] = rec_ref[0, 0] - (fit_re * mre - fit_im * mim)
    prim_ref[0, 1] = rec_ref[0, 1] - (fit_re * mim + fit_im * mre)


def per_device(recorded, receiver_kernel, source_kernel):
    rows, width = recorded.shape[2], recorded.shape[3]
    panels = lax.axis_size("panel")
    sources = rows * panels
    cols = width // panels
    pad = ((0, 0), (1, 0))
    rtaps = jnp.pad(jnp.flip(receiver_kernel[0].astype(jnp.float32), axis=1), pad)
    staps = jnp.pad(source_kernel[0].astype(jnp.float32), pad)
    bf16 = jnp.bfloat16
    vmem = pl.BlockSpec(memory_space=pltpu.VMEM)
    sem = pltpu.SemaphoreType.DMA((panels,))
    mult, fit = pl.pallas_call(
        functools.partial(exchange_kernel, panels),
        out_shape=(
            jax.ShapeDtypeStruct(recorded.shape, bf16),
            jax.ShapeDtypeStruct((8, LANES), jnp.float32),
        ),
        in_specs=[vmem] * 3,
        out_specs=(vmem, vmem),
        scratch_shapes=[
            pltpu.VMEM((2 * width, 2 * LANES), bf16),
            pltpu.VMEM((2 * sources, 2 * rows), bf16),
            pltpu.VMEM((2 * rows, 2 * width), bf16),
            pltpu.VMEM((2 * cols, 2 * sources), bf16),
            pltpu.VMEM((width, 2 * rows), bf16),
            pltpu.VMEM((panels, cols, 2 * rows), bf16),
            pltpu.VMEM((sources, 2 * cols), bf16),
            pltpu.VMEM((panels, rows, 2 * cols), bf16),
            pltpu.VMEM((8, LANES), jnp.float32),
            pltpu.VMEM((panels, 8, LANES), jnp.float32),
            sem,
            sem,
            sem,
            sem,
            sem,
            sem,
        ],
        compiler_params=pltpu.CompilerParams(collective_id=0, has_side_effects=True, vmem_limit_bytes=56 * 2**20),
        name="exchange",
    )(recorded, rtaps, staps)
    strip = rows // 4
    block = pl.BlockSpec((1, 2, strip, width), lambda i: (0, 0, i, 0))
    return pl.pallas_call(
        subtract_kernel,
        grid=(rows // strip,),
        out_shape=(
            jax.ShapeDtypeStruct(recorded.shape, jnp.float32),
            jax.ShapeDtypeStruct(recorded.shape, bf16),
        ),
        in_specs=[block, block, pl.BlockSpec((8, LANES), lambda i: (0, 0))],
        out_specs=(block, block),
        name="subtract",
    )(recorded, mult, fit)


def solution(mesh):
    placed = (P("freq", None, "panel", None), P("freq", None, None), P("freq", None, None))
    return jax.shard_map(
        per_device,
        mesh=mesh,
        in_specs=placed,
        out_specs=(P("freq", None, "panel", None), P("freq", None, "panel", None)),
        check_vma=False,
    )
```

```python
import functools

import jax
import jax.numpy as jnp
from jax import lax
from jax.experimental import pallas as pl
from jax.experimental.pallas import tpu as pltpu
from jax.sharding import PartitionSpec as P

MESH = pl.DeviceIdType.MESH
LANES = 128
GROUP = 256
STRIP = 16
STRIPS = 4


def spread(taps_ref, padded, comp, flipped):
    length = padded.shape[1]
    rows = [padded[comp : comp + 1, at : at + LANES] for at in range(0, length, LANES)]
    if not flipped:
        return jnp.broadcast_to(jnp.concatenate(rows, axis=1), (STRIP, length))
    i = lax.broadcasted_iota(jnp.int32, (LANES, LANES), 0)
    j = lax.broadcasted_iota(jnp.int32, (LANES, LANES), 1)
    swap = jnp.where(i + j == LANES - 1, 1.0, 0.0).astype(jnp.bfloat16)
    tall = jnp.concatenate([jnp.broadcast_to(r, (STRIP, LANES)) for r in rows[::-1]], axis=0)
    tall = jnp.dot(tall.astype(jnp.bfloat16), swap, preferred_element_type=jnp.float32)
    return jnp.concatenate([tall[at : at + STRIP] for at in range(0, tall.shape[0], STRIP)], axis=1)


def skew(taps_ref, padded, flipped, block, band_ref):
    length = padded.shape[1]
    padded[...] = jnp.zeros_like(padded)
    padded[:, 0 : length - 1] = taps_ref[0].astype(jnp.float32)
    row = lax.broadcasted_iota(jnp.int32, (STRIP, length), 0)
    for comp in range(2):
        x = spread(taps_ref, padded, comp, flipped)
        step = 1
        while step < STRIP:
            x = jnp.where((row & step) != 0, pltpu.roll(x, step, 1), x)
            step *= 2
        lane0 = comp * block
        for s in range(0, LANES, STRIP):
            shift = (s - (LANES - block) + (0 if flipped else 1)) % length
            y = (pltpu.roll(x, shift, 1) if shift else x).astype(jnp.bfloat16)
            for m in range(length // LANES):
                at = length - LANES * (m + 1)
                band_ref[m * LANES + s : m * LANES + s + STRIP, lane0 : lane0 + block] = y[:, at : at + block]


def exchange_kernel(
    panels,
    rec_hbm,
    rtaps_hbm,
    staps_hbm,
    rec_ref,
    mult_ref,
    fit_ref,
    rtaps_ref,
    staps_ref,
    load_sem,
    padded,
    band_r,
    band_s,
    w1,
    w2,
    foc,
    foc_in,
    mul,
    mul_in,
    sums,
    sums_in,
    send1,
    recv1,
    send2,
    recv2,
    send3,
    recv3,
):
    me = lax.axis_index("panel")
    rows, width = rec_ref.shape[2], rec_ref.shape[3]
    sources = rows * panels
    cols = width // panels
    halves, hc = foc_in.shape[0], foc_in.shape[2]
    nt = (((1,), (1,)), ((), ()))

    def order(n, own, groups):
        side = groups // 2
        half = lax.rem(own // side + 1 + n // side, 2)
        return half * side + lax.rem(own + 1 + n, side)

    def peer(o):
        return lax.rem(me + o, panels)

    loads = [
        pltpu.make_async_copy(src, dst, load_sem.at[i])
        for i, (src, dst) in enumerate(
            ((rtaps_hbm, rtaps_ref), (rec_hbm, rec_ref), (staps_hbm, staps_ref))
        )
    ]
    for load in loads:
        load.start()

    barrier = pltpu.get_barrier_semaphore()

    @pl.loop(1, panels)
    def _(o):
        pl.semaphore_signal(barrier, inc=1, device_id={"panel": peer(o)}, device_id_type=MESH)

    loads[0].wait()
    skew(rtaps_ref, padded, True, LANES, band_r)
    loads[1].wait()
    for kb in range(width // LANES):
        re = rec_ref[0, 0, :, kb * LANES : (kb + 1) * LANES].astype(jnp.bfloat16)
        im = rec_ref[0, 1, :, kb * LANES : (kb + 1) * LANES].astype(jnp.bfloat16)
        at = 2 * kb * LANES
        w1[0:rows, at : at + LANES] = re
        w1[0:rows, at + LANES : at + 2 * LANES] = -im
        w1[rows : 2 * rows, at : at + LANES] = im
        w1[rows : 2 * rows, at + LANES : at + 2 * LANES] = re

    pl.semaphore_wait(barrier, panels - 1)

    def copy1(h, dest, src):
        return pltpu.make_async_remote_copy(
            src_ref=foc.at[pl.ds(pl.multiple_of(dest * cols + h * hc, hc), hc), :],
            dst_ref=foc_in.at[h, src],
            send_sem=send1.at[h, dest],
            recv_sem=recv1.at[h, src],
            device_id={"panel": dest},
            device_id_type=MESH,
        )

    def copy2(h, dest, src):
        return pltpu.make_async_remote_copy(
            src_ref=mul.at[h, pl.ds(pl.multiple_of(dest * rows, rows), rows), :],
            dst_ref=mul_in.at[h, src],
            send_sem=send2.at[h, dest],
            recv_sem=recv2.at[h, src],
            device_id={"panel": dest},
            device_id_type=MESH,
        )

    def copy3(dest, src):
        return pltpu.make_async_remote_copy(
            src_ref=sums,
            dst_ref=sums_in.at[src],
            send_sem=send3.at[dest],
            recv_sem=recv3.at[src],
            device_id={"panel": dest},
            device_id_type=MESH,
        )

    groups1 = width // GROUP
    per1 = GROUP // cols
    own1 = me // per1

    @pl.loop(0, groups1)
    def _(n):
        g = order(n, own1, groups1)
        first = pl.multiple_of(g * GROUP, GROUP)
        lhs = jnp.concatenate(
            [
                band_r[pl.ds(pl.multiple_of(width - LANES * (kb + 1) + first, LANES), GROUP), :]
                for kb in range(width // LANES)
            ],
            axis=1,
        )
        out = lax.dot_general(lhs, w1[...], nt, preferred_element_type=jnp.float32)
        foc[pl.ds(first, GROUP), :] = out.astype(jnp.bfloat16)
        for d in range(per1):
            dest = g * per1 + d

            @pl.when(dest != me)
            def _():
                copy1(0, dest, me).start()

    for h in range(1, halves):

        @pl.loop(0, groups1)
        def _(n):
            for d in range(per1):
                dest = order(n, own1, groups1) * per1 + d

                @pl.when(dest != me)
                def _():
                    copy1(h, dest, me).start()

    for h in range(halves):
        foc_in[h, me] = foc[pl.ds(pl.multiple_of(me * cols + h * hc, hc), hc), :]
    loads[2].wait()
    skew(staps_ref, padded, False, rows, band_s)

    groups2 = sources // GROUP
    per2 = GROUP // rows
    own2 = me // per2
    lane = lax.broadcasted_iota(jnp.int32, (hc, 2 * rows), 1)
    for h in range(halves):

        @pl.loop(1, panels)
        def _(o):
            copy1(h, peer(o), peer(o)).wait_recv()

        for j in range(panels):
            x = foc_in[h, j]
            at = 2 * rows * j
            w2[0:hc, at : at + 2 * rows] = jnp.where(lane < rows, x, -x)
            w2[hc : 2 * hc, at : at + 2 * rows] = jnp.concatenate([x[:, rows:], x[:, :rows]], axis=1)

        @pl.loop(0, groups2)
        def _(n):
            g = order(n, own2, groups2)
            first = pl.multiple_of(g * GROUP, GROUP)
            lhs = jnp.concatenate(
                [
                    band_s[pl.ds(pl.multiple_of(sources - rows * (jb + 1) + first, rows), GROUP), :]
                    for jb in range(panels)
                ],
                axis=1,
            )
            out = lax.dot_general(lhs, w2[...], nt, preferred_element_type=jnp.float32)
            mul[h, pl.ds(first, GROUP), :] = out.astype(jnp.bfloat16)
            for d in range(per2):
                dest = g * per2 + d

                @pl.when(dest != me)
                def _():
                    copy2(h, dest, me).start()

        mul_in[h, me] = mul[h, pl.ds(pl.multiple_of(me * rows, rows), rows), :]

    def fold(v):
        return jnp.sum(v, axis=0, keepdims=True)

    chunks = width // LANES
    near = LANES // cols

    def gather(n, acc):
        cb = order(n, me // near, chunks)
        blocks = []
        for d in range(near):
            src = cb * near + d

            @pl.when(src != me)
            def _():
                for h in range(halves):
                    copy2(h, src, src).wait_recv()

            blocks += [mul_in[h, src] for h in range(halves)]
        mre = jnp.concatenate([b[:, :hc] for b in blocks], axis=1)
        mim = jnp.concatenate([b[:, hc:] for b in blocks], axis=1)
        at = pl.ds(pl.multiple_of(cb * LANES, LANES), LANES)
        mult_ref[0, 0, :, at] = mre
        mult_ref[0, 1, :, at] = mim
        mre = mre.astype(jnp.float32)
        mim = mim.astype(jnp.float32)
        pre = rec_ref[0, 0, :, at]
        pim = rec_ref[0, 1, :, at]
        return (
            acc[0] + fold(mre * pre + mim * pim),
            acc[1] + fold(mre * pim - mim * pre),
            acc[2] + fold(mre * mre + mim * mim),
        )

    zero = jnp.zeros((1, LANES), jnp.float32)
    num_re, num_im, energy = lax.fori_loop(0, chunks, gather, (zero, zero, zero))
    part = jnp.concatenate([num_re, num_im, energy, jnp.zeros((5, LANES), jnp.float32)], axis=0)
    sums[...] = part
    sums_in[me] = part

    @pl.loop(1, panels)
    def _(o):
        copy3(peer(o), me).start()

    @pl.loop(1, panels)
    def _(o):
        for h in range(halves):
            copy1(h, peer(o), me).wait_send()
            copy2(h, peer(o), me).wait_send()

    @pl.loop(1, panels)
    def _(o):
        copy3(peer(o), peer(o)).wait_recv()

    @pl.loop(1, panels)
    def _(o):
        copy3(peer(o), me).wait_send()

    total = jnp.sum(jnp.sum(sums_in[...], axis=0), axis=1, keepdims=True)
    fit = total[0:2, :] / (total[2:3, :] + 1e-06)
    fit_ref[...] = jnp.broadcast_to(
        jnp.concatenate([fit, jnp.zeros((6, 1), jnp.float32)], axis=0), (8, LANES)
    )


def subtract_kernel(rec_ref, mult_ref, fit_ref, prim_hbm, mult_hbm, prim, sem):
    mult_out = pltpu.make_async_copy(mult_ref, mult_hbm, sem.at[0])
    mult_out.start()
    fit_re = fit_ref[0:1, 0:1]
    fit_im = fit_ref[1:2, 0:1]
    rows = rec_ref.shape[2]
    strip = rows // STRIPS
    outs = []
    for i in range(STRIPS):
        at = slice(i * strip, (i + 1) * strip)
        mre = mult_ref[0, 0, at, :].astype(jnp.float32)
        mim = mult_ref[0, 1, at, :].astype(jnp.float32)
        prim[0, 0, at, :] = rec_ref[0, 0, at, :] - (fit_re * mre - fit_im * mim)
        prim[0, 1, at, :] = rec_ref[0, 1, at, :] - (fit_re * mim + fit_im * mre)
        out = pltpu.make_async_copy(prim.at[:, :, at, :], prim_hbm.at[:, :, at, :], sem.at[i + 1])
        out.start()
        outs.append(out)
    for out in outs:
        out.wait()
    mult_out.wait()


def per_device(recorded, receiver_kernel, source_kernel):
    rows, width = recorded.shape[2], recorded.shape[3]
    panels = lax.axis_size("panel")
    sources = rows * panels
    cols = width // panels
    bf16 = jnp.bfloat16
    vmem = pl.BlockSpec(memory_space=pltpu.VMEM)
    hc = min(cols, LANES // 2)
    halves = cols // hc
    sem = pltpu.SemaphoreType.DMA((panels,))
    sems = pltpu.SemaphoreType.DMA((halves, panels))
    hbm = pl.BlockSpec(memory_space=pltpu.HBM)
    rec, mult, fit = pl.pallas_call(
        functools.partial(exchange_kernel, panels),
        out_shape=(
            jax.ShapeDtypeStruct(recorded.shape, jnp.float32),
            jax.ShapeDtypeStruct(recorded.shape, bf16),
            jax.ShapeDtypeStruct((8, LANES), jnp.float32),
        ),
        in_specs=[hbm] * 3,
        out_specs=(vmem, vmem, vmem),
        scratch_shapes=[
            pltpu.VMEM(receiver_kernel.shape, bf16),
            pltpu.VMEM(source_kernel.shape, bf16),
            pltpu.SemaphoreType.DMA((3,)),
            pltpu.VMEM((2, 2 * width), jnp.float32),
            pltpu.VMEM((2 * width, 2 * LANES), bf16),
            pltpu.VMEM((2 * sources, 2 * rows), bf16),
            pltpu.VMEM((2 * rows, 2 * width), bf16),
            pltpu.VMEM((2 * hc, 2 * sources), bf16),
            pltpu.VMEM((width, 2 * rows), bf16),
            pltpu.VMEM((halves, panels, hc, 2 * rows), bf16),
            pltpu.VMEM((halves, sources, 2 * hc), bf16),
            pltpu.VMEM((halves, panels, rows, 2 * hc), bf16),
            pltpu.VMEM((8, LANES), jnp.float32),
            pltpu.VMEM((panels, 8, LANES), jnp.float32),
            sems,
            sems,
            sems,
            sems,
            sem,
            sem,
        ],
        compiler_params=pltpu.CompilerParams(collective_id=0, has_side_effects=True, vmem_limit_bytes=32 * 2**20),
        name="exchange",
    )(recorded, receiver_kernel, source_kernel)
    return pl.pallas_call(
        subtract_kernel,
        out_shape=(
            jax.ShapeDtypeStruct(recorded.shape, jnp.float32),
            jax.ShapeDtypeStruct(recorded.shape, bf16),
        ),
        in_specs=[vmem] * 3,
        out_specs=(hbm, hbm),
        scratch_shapes=[pltpu.VMEM(recorded.shape, jnp.float32), pltpu.SemaphoreType.DMA((STRIPS + 1,))],
        compiler_params=pltpu.CompilerParams(vmem_limit_bytes=12 * 2**20),
        name="subtract",
    )(rec, mult, fit)


def solution(mesh):
    placed = (P("freq", None, "panel", None), P("freq", None, None), P("freq", None, None))
    return jax.shard_map(
        per_device,
        mesh=mesh,
        in_specs=placed,
        out_specs=(P("freq", None, "panel", None), P("freq", None, "panel", None)),
        check_vma=False,
    )
```

```python
import functools

import jax
import jax.numpy as jnp
from jax import lax
from jax.experimental import pallas as pl
from jax.experimental.pallas import tpu as pltpu
from jax.sharding import PartitionSpec as P

MESH = pl.DeviceIdType.MESH
LANES = 128
GROUP = 256
STRIP = 16
STRIPS = 4


def spread(taps_ref, padded, comp, flipped):
    length = padded.shape[1]
    rows = [padded[comp : comp + 1, at : at + LANES] for at in range(0, length, LANES)]
    if not flipped:
        return jnp.broadcast_to(jnp.concatenate(rows, axis=1), (STRIP, length))
    i = lax.broadcasted_iota(jnp.int32, (LANES, LANES), 0)
    j = lax.broadcasted_iota(jnp.int32, (LANES, LANES), 1)
    swap = jnp.where(i + j == LANES - 1, 1.0, 0.0).astype(jnp.bfloat16)
    tall = jnp.concatenate([jnp.broadcast_to(r, (STRIP, LANES)) for r in rows[::-1]], axis=0)
    tall = jnp.dot(tall.astype(jnp.bfloat16), swap, preferred_element_type=jnp.float32)
    return jnp.concatenate([tall[at : at + STRIP] for at in range(0, tall.shape[0], STRIP)], axis=1)


def skew(taps_ref, padded, flipped, block, band_ref):
    length = padded.shape[1]
    padded[...] = jnp.zeros_like(padded)
    padded[:, 0 : length - 1] = taps_ref[0].astype(jnp.float32)
    row = lax.broadcasted_iota(jnp.int32, (STRIP, length), 0)
    for comp in range(2):
        x = spread(taps_ref, padded, comp, flipped)
        step = 1
        while step < STRIP:
            x = jnp.where((row & step) != 0, pltpu.roll(x, step, 1), x)
            step *= 2
        lane0 = comp * block
        for s in range(0, LANES, STRIP):
            shift = (s - (LANES - block) + (0 if flipped else 1)) % length
            y = (pltpu.roll(x, shift, 1) if shift else x).astype(jnp.bfloat16)
            for m in range(length // LANES):
                at = length - LANES * (m + 1)
                band_ref[m * LANES + s : m * LANES + s + STRIP, lane0 : lane0 + block] = y[:, at : at + block]


def exchange_kernel(
    panels,
    rec_hbm,
    rtaps_hbm,
    staps_hbm,
    rec_ref,
    mult_ref,
    fit_ref,
    rtaps_ref,
    staps_ref,
    load_sem,
    padded,
    band_r,
    band_s,
    w1,
    w2,
    foc,
    foc_in,
    mul,
    mul_in,
    sums,
    sums_in,
    send1,
    recv1,
    send2,
    recv2,
    send3,
    recv3,
):
    me = lax.axis_index("panel")
    rows, width = rec_ref.shape[2], rec_ref.shape[3]
    sources = rows * panels
    cols = width // panels
    halves, hc = foc_in.shape[0], foc_in.shape[2]
    nt = (((1,), (1,)), ((), ()))

    def order(n, own, groups):
        side = groups // 2
        half = lax.rem(own // side + 1 + n // side, 2)
        return half * side + lax.rem(own + 1 + n, side)

    def peer(o):
        return lax.rem(me + o, panels)

    loads = [
        pltpu.make_async_copy(src, dst, load_sem.at[i])
        for i, (src, dst) in enumerate(
            ((rtaps_hbm, rtaps_ref), (rec_hbm, rec_ref), (staps_hbm, staps_ref))
        )
    ]
    for load in loads:
        load.start()

    barrier = pltpu.get_barrier_semaphore()

    @pl.loop(1, panels)
    def _(o):
        pl.semaphore_signal(barrier, inc=1, device_id={"panel": peer(o)}, device_id_type=MESH)

    loads[0].wait()
    skew(rtaps_ref, padded, True, LANES, band_r)
    loads[1].wait()
    for kb in range(width // LANES):
        re = rec_ref[0, 0, :, kb * LANES : (kb + 1) * LANES].astype(jnp.bfloat16)
        im = rec_ref[0, 1, :, kb * LANES : (kb + 1) * LANES].astype(jnp.bfloat16)
        at = 2 * kb * LANES
        w1[0:rows, at : at + LANES] = re
        w1[0:rows, at + LANES : at + 2 * LANES] = -im
        w1[rows : 2 * rows, at : at + LANES] = im
        w1[rows : 2 * rows, at + LANES : at + 2 * LANES] = re

    pl.semaphore_wait(barrier, panels - 1)

    def copy1(h, dest, src):
        return pltpu.make_async_remote_copy(
            src_ref=foc.at[pl.ds(pl.multiple_of(dest * cols + h * hc, hc), hc), :],
            dst_ref=foc_in.at[h, src],
            send_sem=send1.at[h, dest],
            recv_sem=recv1.at[h, src],
            device_id={"panel": dest},
            device_id_type=MESH,
        )

    def copy2(h, dest, src):
        return pltpu.make_async_remote_copy(
            src_ref=mul.at[h, pl.ds(pl.multiple_of(dest * rows, rows), rows), :],
            dst_ref=mul_in.at[h, src],
            send_sem=send2.at[h, dest],
            recv_sem=recv2.at[h, src],
            device_id={"panel": dest},
            device_id_type=MESH,
        )

    def copy3(dest, src):
        return pltpu.make_async_remote_copy(
            src_ref=sums,
            dst_ref=sums_in.at[src],
            send_sem=send3.at[dest],
            recv_sem=recv3.at[src],
            device_id={"panel": dest},
            device_id_type=MESH,
        )

    groups1 = width // GROUP
    per1 = GROUP // cols
    own1 = me // per1

    @pl.loop(0, groups1)
    def _(n):
        g = order(n, own1, groups1)
        first = pl.multiple_of(g * GROUP, GROUP)
        lhs = jnp.concatenate(
            [
                band_r[pl.ds(pl.multiple_of(width - LANES * (kb + 1) + first, LANES), GROUP), :]
                for kb in range(width // LANES)
            ],
            axis=1,
        )
        out = lax.dot_general(lhs, w1[...], nt, preferred_element_type=jnp.float32)
        foc[pl.ds(first, GROUP), :] = out.astype(jnp.bfloat16)
        for d in range(per1):
            dest = g * per1 + d

            @pl.when(dest != me)
            def _():
                copy1(0, dest, me).start()

    for h in range(1, halves):

        @pl.loop(0, groups1)
        def _(n):
            for d in range(per1):
                dest = order(n, own1, groups1) * per1 + d

                @pl.when(dest != me)
                def _():
                    copy1(h, dest, me).start()

    for h in range(halves):
        foc_in[h, me] = foc[pl.ds(pl.multiple_of(me * cols + h * hc, hc), hc), :]
    loads[2].wait()
    skew(staps_ref, padded, False, rows, band_s)

    groups2 = sources // GROUP
    per2 = GROUP // rows
    own2 = me // per2
    lane = lax.broadcasted_iota(jnp.int32, (hc, 2 * rows), 1)
    for h in range(halves):

        @pl.loop(1, panels)
        def _(o):
            copy1(h, peer(o), peer(o)).wait_recv()

        for j in range(panels):
            x = foc_in[h, j]
            at = 2 * rows * j
            w2[0:hc, at : at + 2 * rows] = jnp.where(lane < rows, x, -x)
            w2[hc : 2 * hc, at : at + 2 * rows] = jnp.concatenate([x[:, rows:], x[:, :rows]], axis=1)

        @pl.loop(0, groups2)
        def _(n):
            g = order(n, own2, groups2)
            first = pl.multiple_of(g * GROUP, GROUP)
            lhs = jnp.concatenate(
                [
                    band_s[pl.ds(pl.multiple_of(sources - rows * (jb + 1) + first, rows), GROUP), :]
                    for jb in range(panels)
                ],
                axis=1,
            )
            out = lax.dot_general(lhs, w2[...], nt, preferred_element_type=jnp.float32)
            mul[h, pl.ds(first, GROUP), :] = out.astype(jnp.bfloat16)
            for d in range(per2):
                dest = g * per2 + d

                @pl.when(dest != me)
                def _():
                    copy2(h, dest, me).start()

        mul_in[h, me] = mul[h, pl.ds(pl.multiple_of(me * rows, rows), rows), :]

    def fold(v):
        return jnp.sum(v, axis=0, keepdims=True)

    chunks = width // LANES
    near = LANES // cols

    def gather(n, acc):
        cb = order(n, me // near, chunks)
        blocks = []
        for d in range(near):
            src = cb * near + d

            @pl.when(src != me)
            def _():
                for h in range(halves):
                    copy2(h, src, src).wait_recv()

            blocks += [mul_in[h, src] for h in range(halves)]
        mre = jnp.concatenate([b[:, :hc] for b in blocks], axis=1)
        mim = jnp.concatenate([b[:, hc:] for b in blocks], axis=1)
        at = pl.ds(pl.multiple_of(cb * LANES, LANES), LANES)
        mult_ref[0, 0, :, at] = mre
        mult_ref[0, 1, :, at] = mim
        mre = mre.astype(jnp.float32)
        mim = mim.astype(jnp.float32)
        pre = rec_ref[0, 0, :, at]
        pim = rec_ref[0, 1, :, at]
        return (
            acc[0] + fold(mre * pre + mim * pim),
            acc[1] + fold(mre * pim - mim * pre),
            acc[2] + fold(mre * mre + mim * mim),
        )

    zero = jnp.zeros((1, LANES), jnp.float32)
    num_re, num_im, energy = lax.fori_loop(0, chunks, gather, (zero, zero, zero))
    part = jnp.concatenate([num_re, num_im, energy, jnp.zeros((5, LANES), jnp.float32)], axis=0)
    sums[...] = part
    sums_in[me] = part

    @pl.loop(1, panels)
    def _(o):
        copy3(peer(o), me).start()

    @pl.loop(1, panels)
    def _(o):
        for h in range(halves):
            copy1(h, peer(o), me).wait_send()
            copy2(h, peer(o), me).wait_send()

    @pl.loop(1, panels)
    def _(o):
        copy3(peer(o), peer(o)).wait_recv()

    @pl.loop(1, panels)
    def _(o):
        copy3(peer(o), me).wait_send()

    total = jnp.sum(jnp.sum(sums_in[...], axis=0), axis=1, keepdims=True)
    fit = total[0:2, :] / (total[2:3, :] + 1e-06)
    fit_ref[...] = jnp.broadcast_to(
        jnp.concatenate([fit, jnp.zeros((6, 1), jnp.float32)], axis=0), (8, LANES)
    )


def subtract_kernel(rec_ref, mult_ref, fit_ref, prim_hbm, mult_hbm, prim, sem):
    mult_out = pltpu.make_async_copy(mult_ref, mult_hbm, sem.at[0])
    mult_out.start()
    fit_re = fit_ref[0:1, 0:1]
    fit_im = fit_ref[1:2, 0:1]
    rows = rec_ref.shape[2]
    strip = rows // STRIPS
    outs = []
    for i in range(STRIPS):
        at = slice(i * strip, (i + 1) * strip)
        mre = mult_ref[0, 0, at, :].astype(jnp.float32)
        mim = mult_ref[0, 1, at, :].astype(jnp.float32)
        prim[0, 0, at, :] = rec_ref[0, 0, at, :] - (fit_re * mre - fit_im * mim)
        prim[0, 1, at, :] = rec_ref[0, 1, at, :] - (fit_re * mim + fit_im * mre)
        out = pltpu.make_async_copy(prim.at[:, :, at, :], prim_hbm.at[:, :, at, :], sem.at[i + 1])
        out.start()
        outs.append(out)
    for out in outs:
        out.wait()
    mult_out.wait()


def per_device(recorded, receiver_kernel, source_kernel):
    rows, width = recorded.shape[2], recorded.shape[3]
    panels = lax.axis_size("panel")
    sources = rows * panels
    cols = width // panels
    bf16 = jnp.bfloat16
    vmem = pl.BlockSpec(memory_space=pltpu.VMEM)
    hc = min(cols, LANES // 2)
    halves = cols // hc
    sem = pltpu.SemaphoreType.DMA((panels,))
    sems = pltpu.SemaphoreType.DMA((halves, panels))
    hbm = pl.BlockSpec(memory_space=pltpu.HBM)
    rec, mult, fit = pl.pallas_call(
        functools.partial(exchange_kernel, panels),
        out_shape=(
            jax.ShapeDtypeStruct(recorded.shape, jnp.float32),
            jax.ShapeDtypeStruct(recorded.shape, bf16),
            jax.ShapeDtypeStruct((8, LANES), jnp.float32),
        ),
        in_specs=[hbm] * 3,
        out_specs=(vmem, vmem, vmem),
        scratch_shapes=[
            pltpu.VMEM(receiver_kernel.shape, bf16),
            pltpu.VMEM(source_kernel.shape, bf16),
            pltpu.SemaphoreType.DMA((3,)),
            pltpu.VMEM((2, 2 * width), jnp.float32),
            pltpu.VMEM((2 * width, 2 * LANES), bf16),
            pltpu.VMEM((2 * sources, 2 * rows), bf16),
            pltpu.VMEM((2 * rows, 2 * width), bf16),
            pltpu.VMEM((2 * hc, 2 * sources), bf16),
            pltpu.VMEM((width, 2 * rows), bf16),
            pltpu.VMEM((halves, panels, hc, 2 * rows), bf16),
            pltpu.VMEM((halves, sources, 2 * hc), bf16),
            pltpu.VMEM((halves, panels, rows, 2 * hc), bf16),
            pltpu.VMEM((8, LANES), jnp.float32),
            pltpu.VMEM((panels, 8, LANES), jnp.float32),
            sems,
            sems,
            sems,
            sems,
            sem,
            sem,
        ],
        compiler_params=pltpu.CompilerParams(collective_id=0, has_side_effects=True, vmem_limit_bytes=50 * 2**20),
        name="exchange",
    )(
        *(pltpu.with_memory_space_constraint(x, pltpu.HBM) for x in (recorded, receiver_kernel, source_kernel))
    )
    return pl.pallas_call(
        subtract_kernel,
        out_shape=(
            jax.ShapeDtypeStruct(recorded.shape, jnp.float32),
            jax.ShapeDtypeStruct(recorded.shape, bf16),
        ),
        in_specs=[vmem] * 3,
        out_specs=(hbm, hbm),
        scratch_shapes=[pltpu.VMEM(recorded.shape, jnp.float32), pltpu.SemaphoreType.DMA((STRIPS + 1,))],
        compiler_params=pltpu.CompilerParams(vmem_limit_bytes=12 * 2**20),
        name="subtract",
    )(rec, mult, fit)


def solution(mesh):
    placed = (P("freq", None, "panel", None), P("freq", None, None), P("freq", None, None))
    return jax.shard_map(
        per_device,
        mesh=mesh,
        in_specs=placed,
        out_specs=(P("freq", None, "panel", None), P("freq", None, "panel", None)),
        check_vma=False,
    )
```
